32 devices in a mesh: ep: 8 (over y, x, core), tp: 4 (over z).
Axes of the slice: x: 2, y: 2, z: 4, core: 2. Of those that a mesh axis runs over, the one named last changes fastest.
Arguments:
- tokens: bfloat16 [5120, 2048], P('ep'), may hold values from -6 to 6
- norm1_gain: float32 [2048], replicated, may hold values from 0.1 to 1.9
- w_qkv: bfloat16 [3, 2048, 2048], P(None, None, 'tp'), may hold values from -0.125 to 0.125
- b_qkv: bfloat16 [3, 16, 128], P(None, 'tp'), may hold values from -3 to 3
- w_out: bfloat16 [2048, 2048], P('tp'), may hold values from -1.25 to 1.25
- norm2_gain: float32 [2048], replicated, may hold values from 0.1 to 1.9
- w_router: bfloat16 [2048, 8], replicated, may hold values from -0.0625 to 0.0625
- w_sgate: bfloat16 [2048], replicated, may hold values from -0.125 to 0.125
- w_shared_gu: bfloat16 [2, 2048, 5632], P(None, None, 'tp'), may hold values from -0.125 to 0.125
- w_shared_down: bfloat16 [5632, 2048], P('tp'), may hold values from -0.15625 to 0.15625
- w_expert_gu: bfloat16 [8, 2, 2048, 1408], P('ep', None, None, 'tp'), may hold values from -0.125 to 0.125
- w_expert_down: bfloat16 [8, 1408, 2048], P('ep', 'tp'), may hold values from -0.3125 to 0.3125
- routes: int32 [5120, 4], P('ep'), may hold values from 0 to 7, all different within a row; in each aligned block of 640 rows (0 to 639, 640 to 1279, ...) at most 400 rows name the same one
- grad_out: bfloat16 [5120, 2048], P('ep'), may hold values from -6 to 6
Outputs:
- output: bfloat16 [5120, 2048], P(('ep', 'tp'))
- grad_tokens: float32 [5120, 2048], P(('ep', 'tp'))
- grad_norm1_gain: float32 [2048], P('ep')
- grad_w_qkv: float32 [3, 2048, 2048], P(None, 'ep', 'tp')
- grad_b_qkv: float32 [3, 16, 128], P(None, 'tp', 'ep')
- grad_w_out: float32 [2048, 2048], P('tp', 'ep')
- grad_norm2_gain: float32 [2048], P('ep')
- grad_w_router: float32 [2048, 8], P('ep')
- grad_w_sgate: float32 [2048], P('ep')
- grad_w_shared_gu: float32 [2, 2048, 5632], P(None, 'ep', 'tp')
- grad_w_shared_down: float32 [5632, 2048], P('tp', 'ep')
- grad_w_expert_gu: float32 [8, 2, 2048, 1408], P('ep', None, None, 'tp')
- grad_w_expert_down: float32 [8, 1408, 2048], P('ep', 'tp')
The draws below stay inside these ranges and needn't reach their ends.
Inputs may be any that keep to these rules, and one draw needn't show every extreme that they name: `routes`: each row names 4 different experts. Among the rows of one sequence no expert is named more than 400 times, and in every draw some expert is named exactly 400 times within some sequence.
All inputs are finite; a program needn't handle non-finite values.
Results may differ from the reference program's by a relative error of at most 0.024.
Values may be sent and summed in bfloat16 or wider, within the bound.
A program may use at most 384 MiB of HBM per device.

```python
import math
import jax
import jax.numpy as jnp
import numpy as np
from jax import lax

D = 2048
HEADS = 16
HD = 128
EH = 1408
SH = 5632
TOP = 4
SEQ_LEN = 640
EXPERTS = 8
TOKENS = 5120
CAP = 400
N_EP = 8
N_TP = 4


def levels(rng, shape, pieces, smallest, high):
    def one(position, shards_of):
        heights = jax.random.uniform(jax.random.fold_in(jax.random.fold_in(rng, 6), position), (shards_of,), jnp.float32, smallest / len(pieces), high / len(pieces))
        return jnp.repeat(jnp.exp(heights), shape[position] // shards_of).reshape((-1,) + (1,) * (len(shape) - position - 1))

    factor_of = one(*pieces[0])
    for cut in pieces[1:]:
        factor_of = factor_of * one(*cut)
    return factor_of


def routed_block(stream_key, own, number, rows, count, top, reach, slope):
    sequence = jax.random.permutation(stream_key, count)
    crowded, ordinary = shares(count, rows * top, reach, slope, True), shares(count, rows * top, reach, slope, False)
    places = jnp.arange(count)

    def named(sizes, rotation):
        used = int((sizes > 0).sum())
        fixed = max(1, used // 4)
        shifted = fixed + (places - fixed + rotation * (used - fixed)) % max(1, count - fixed)
        return jnp.zeros((count,), jnp.int32).at[sequence[jnp.where(places < fixed, places, shifted)]].set(jnp.asarray(sizes, jnp.int32))

    sizes = jnp.where(number % 4 == 0, named(crowded, number // 4), named(ordinary, number - number // 4 - 1))
    mixed = jax.random.permutation(jax.random.fold_in(own, 3), count)
    source_of, sink = mixed[0:count // 2 * 2:2], mixed[1:count // 2 * 2:2]
    room = jnp.minimum(sizes[source_of] - 1, reach - sizes[sink]) // 2
    room = jnp.where((source_of == sequence[0]) | (sink == sequence[0]) | (sizes[sink] == 0), 0, jnp.maximum(room, 0))
    shifted = jax.random.randint(jax.random.fold_in(own, 4), (count // 2,), 0, 1 << 20) % (room + 1)
    sizes = sizes.at[source_of].add(-shifted).at[sink].add(shifted)
    items = jnp.searchsorted(jnp.cumsum(sizes), jnp.arange(rows * top), side="right").astype(jnp.int32)
    grid = items.reshape(top, rows).T
    grid = grid[jax.random.permutation(jax.random.fold_in(own, 1), rows)]
    rotation = jax.random.randint(jax.random.fold_in(own, 2), (rows, 1), 0, top)
    return jnp.take_along_axis(grid, (jnp.arange(top)[None, :] + rotation) % top, axis=1)


def shares(number_of, total, limit, skew, full):
    portions = [(1 << 20) // math.isqrt(standing ** skew) + 1 for standing in range(1, number_of + 1)]
    largest = limit if full else min(limit, max(-(-total // number_of), total * portions[0] // sum(portions)))
    least = 1 if total - largest >= number_of - 1 else 0
    given, rest = [largest] + [least] * (number_of - 1), total - largest - least * (number_of - 1)
    while rest > 0:
        free = [i for i in range(1, number_of) if given[i] < largest] or [i for i in range(1, number_of) if given[i] < limit]
        whole, budget = sum([portions[i] for i in free]), rest
        for i in free:
            addition = min(limit - given[i], max(1, budget * portions[i] // whole), rest)
            given[i] = given[i] + addition
            rest = rest - addition
    return np.array(given)


def scatter_about(stream_key, shape, spread, most, shards=(), kind=jnp.bfloat16):
    drawn = jax.random.normal(stream_key, shape, jnp.float32) * spread
    if len(shards) > 0:
        drawn = levels(stream_key, shape, shards, -0.22, 0.18) * drawn
    return jnp.clip(drawn, min=-most, max=most).astype(kind)


def setup_inputs(seed: int = 0) -> dict:
    key_of = jax.random.split(jax.random.key(seed), 15)
    tokens = scatter_about(key_of[0], (TOKENS, D), 1.0, 6.0, ((0, 8),))
    norm1_gain = jnp.clip(1.0 + 0.18 * jax.random.normal(key_of[1], (D,), jnp.float32), 0.1, 1.9)
    w_qkv = scatter_about(key_of[2], (3, D, HEADS * HD), D ** -0.5, 0.125, ((2, 4),))
    b_qkv = scatter_about(key_of[3], (3, HEADS, HD), 0.5, 3.0, ((1, 4),))
    w_out = scatter_about(key_of[4], (HEADS * HD, D), (max(1, HEADS * HD * 8 // SEQ_LEN)) ** -0.5, 1.25, ((0, 4),))
    norm2_gain = jnp.clip(1.0 + 0.18 * jax.random.normal(key_of[5], (D,), jnp.float32), 0.1, 1.9)
    w_router = scatter_about(key_of[6], (D, EXPERTS), (4 * D) ** -0.5, 0.0625)
    w_sgate = scatter_about(key_of[7], (D,), D ** -0.5, 0.125)
    w_shared_gu = scatter_about(key_of[8], (2, D, SH), D ** -0.5, 0.125, ((2, 4),))
    w_shared_down = scatter_about(key_of[9], (SH, D), (SH // 4) ** -0.5, 0.15625, ((0, 4),))
    w_expert_gu = scatter_about(key_of[10], (EXPERTS, 2, D, EH), D ** -0.5, 0.125, ((0, 8), (3, 4)))
    w_expert_down = scatter_about(key_of[11], (EXPERTS, EH, D), (max(1, EH * TOP * TOP // (EXPERTS * EXPERTS))) ** -0.5, 0.3125, ((0, 8), (1, 4)))
    routes_keys = jax.random.split(jax.random.fold_in(key_of[12], 1), TOKENS // SEQ_LEN)
    routes_turns = jax.random.permutation(jax.random.fold_in(key_of[12], 3), TOKENS // SEQ_LEN)
    routes = jax.vmap(lambda own, number: routed_block(jax.random.fold_in(key_of[12], 2), own, number, SEQ_LEN, EXPERTS, TOP, CAP, 2))(routes_keys, routes_turns).reshape((TOKENS, TOP))
    grad_out = scatter_about(key_of[13], (TOKENS, D), 1.0, 6.0, ((0, 8),))
    return dict(tokens=tokens, norm1_gain=norm1_gain, w_qkv=w_qkv, b_qkv=b_qkv, w_out=w_out, norm2_gain=norm2_gain, w_router=w_router, w_sgate=w_sgate, w_shared_gu=w_shared_gu, w_shared_down=w_shared_down, w_expert_gu=w_expert_gu, w_expert_down=w_expert_down, routes=routes, grad_out=grad_out)


@jax.custom_vjp
def low(v):
    return lax.optimization_barrier(v.astype(jnp.bfloat16)).astype(jnp.float32)

@jax.custom_vjp
def low_back(v):
    return v

def low_keep(v):
    return (low(v), None)

def low_pass(kept, grad):
    return (grad,)

def back_keep(v):
    return (v, None)

def back_low(kept, grad):
    return (low(grad),)
low.defvjp(low_keep, low_pass)
low_back.defvjp(back_keep, back_low)
norm_eps = 1e-06
rope_base = 1000000.0
masked_score = -1e+30
highest = lax.Precision.HIGHEST

def rms_norm(hidden, gain_vector):
    inv_scale = lax.rsqrt(lax.optimization_barrier(jnp.mean(hidden * hidden, axis=-1, keepdims=True)) + norm_eps)
    return hidden * inv_scale * gain_vector

def rope_tables(length):
    half_dim = HD // 2
    frequency = rope_base ** (-(jnp.arange(half_dim, dtype=jnp.float32) * 2.0) / HD)
    angles = jnp.arange(length, dtype=jnp.float32)[:, None] * frequency[None, :]
    cosine_table = jnp.concatenate([jnp.cos(angles), jnp.cos(angles)], axis=-1)[:, None, :]
    sine_table = jnp.concatenate([jnp.sin(angles), jnp.sin(angles)], axis=-1)[:, None, :]
    return (cosine_table, sine_table)

def rotate_forward(values, cosine_table, sine_table):
    half_dim = values.shape[-1] // 2
    turned = jnp.concatenate([-values[..., half_dim:], values[..., :half_dim]], axis=-1)
    return values * cosine_table + turned * sine_table

def attend(seq_block):
    queries, key_rows, value_rows = seq_block
    length = queries.shape[0]
    scores = jnp.einsum('qhd,khd->hqk', queries, key_rows, precision=highest) * HD ** (-0.5)
    scores = low_back(scores)
    positions = jnp.arange(length)
    causal = positions[None, :] <= positions[:, None]
    scores = jnp.where(causal[None], scores, masked_score)
    attn_probs = jax.nn.softmax(scores, axis=-1)
    return jnp.einsum('hqk,khd->qhd', low(attn_probs), value_rows, precision=highest)

def expert_block(packed):
    row_block, gate_up, down_proj = packed
    piece_width = EH // N_TP
    summed = jnp.zeros(row_block.shape, row_block.dtype)
    for lane_piece in range(N_TP):
        start = lane_piece * piece_width
        stop = start + piece_width
        lane_rows = low_back(row_block)
        gate_up_out = low_back(jnp.einsum('rd,cdf->crf', lane_rows, gate_up[:, :, start:stop], precision=highest))
        activation = low(jax.nn.silu(gate_up_out[0]) * gate_up_out[1])
        summed = summed + low(low_back(jnp.dot(activation, down_proj[start:stop], precision=highest)))
    return summed

def slot_plan(routes):
    pair_experts = routes.reshape(N_EP, SEQ_LEN * TOP)
    choose = (pair_experts[:, :, None] == jnp.arange(EXPERTS, dtype=jnp.int32)[None, None, :]).astype(jnp.int32)
    before = jnp.cumsum(choose, axis=1) - choose
    slot_number = lax.optimization_barrier(jnp.sum(before * choose, axis=2))
    group_index = jnp.arange(N_EP, dtype=jnp.int32)[:, None]
    slot_dest = (pair_experts * (N_EP * CAP) + group_index * CAP + slot_number).reshape(-1).astype(jnp.int32)
    pair_count = TOKENS * TOP
    slot_owner = jnp.full((EXPERTS * N_EP * CAP,), pair_count, jnp.int32).at[slot_dest].set(jnp.arange(pair_count, dtype=jnp.int32))
    return (slot_dest, (slot_owner // TOP).astype(jnp.int32))

def reference(tokens, norm1_gain, w_qkv, b_qkv, w_out, norm2_gain, w_router, w_sgate, w_shared_gu, w_shared_down, w_expert_gu, w_expert_down, routes, grad_out):
    slot_dest, token_source = slot_plan(routes)

    def forward(residual, gain_one, qkv_weight, qkv_bias, out_weight, gain_two, router_weight, sgate_weight, shared_gate_up, shared_down, expert_gate_up, expert_down):
        hidden_one = low(rms_norm(residual, gain_one))
        qkv_pre = jnp.einsum('td,cde->cte', hidden_one, qkv_weight, precision=highest)
        qkv_pre = low_back(qkv_pre + qkv_bias.reshape(3, 1, HEADS * HD))
        shaped = qkv_pre.reshape(3, N_EP, SEQ_LEN, HEADS, HD)
        cosine_table, sine_table = rope_tables(SEQ_LEN)
        queries = low(rotate_forward(shaped[0], cosine_table, sine_table))
        key_rows = low(rotate_forward(shaped[1], cosine_table, sine_table))
        value_rows = low(shaped[2])
        attn_mixed = lax.map(jax.checkpoint(attend), (queries, key_rows, value_rows))
        attn_mixed = low(low_back(attn_mixed.reshape(TOKENS, HEADS * HD)))
        attn_out = low_back(jnp.dot(attn_mixed, out_weight, precision=highest))
        hidden = residual + attn_out
        hidden_two = low(rms_norm(hidden, gain_two))
        logits = low_back(jnp.dot(hidden_two, router_weight, precision=highest))
        router_probs = jax.nn.softmax(logits, axis=-1)
        gate_values = jnp.take_along_axis(router_probs, routes, axis=1)
        sgate_logit = low_back(jnp.dot(hidden_two, sgate_weight, precision=highest))
        shared_gu = low_back(jnp.einsum('td,cdf->ctf', hidden_two, shared_gate_up, precision=highest))
        shared_act = low(jax.nn.silu(shared_gu[0]) * shared_gu[1])
        shared_out = low_back(jnp.dot(shared_act, shared_down, precision=highest))
        padded = jnp.concatenate([hidden_two, jnp.zeros((1, D), hidden_two.dtype)], axis=0)
        expert_rows = padded[token_source].reshape(EXPERTS, N_EP * CAP, D)
        expert_out = lax.map(jax.checkpoint(expert_block), (expert_rows, expert_gate_up, expert_down))
        picked = expert_out.reshape(-1, D)[slot_dest].reshape(TOKENS, TOP, D)
        expert_sum = lax.optimization_barrier(jnp.sum(gate_values[:, :, None] * picked, axis=1))
        return hidden + jax.nn.sigmoid(sgate_logit)[:, None] * shared_out + expert_sum
    floats = tuple((argument.astype(jnp.float32) for argument in (tokens, norm1_gain, w_qkv, b_qkv, w_out, norm2_gain, w_router, w_sgate, w_shared_gu, w_shared_down, w_expert_gu, w_expert_down)))
    output, pullback = jax.vjp(forward, *floats)
    gradients = pullback(grad_out.astype(jnp.float32))
    return (output.astype(jnp.bfloat16), gradients[0], gradients[1], gradients[2], gradients[3], gradients[4], gradients[5], gradients[6], gradients[7], gradients[8], gradients[9], gradients[10], gradients[11])
```

```python
import functools

import jax
import jax.numpy as jnp
from jax import lax
from jax.experimental import pallas as pl
from jax.experimental.pallas import tpu as pltpu
from jax.sharding import PartitionSpec as P

norm_eps = 1e-06
rope_base = 1000000.0
masked_score = -1e30


def contract(left_side, right_side, left_dim, right_dim):
    return lax.dot_general(
        left_side,
        right_side,
        (((left_dim,), (right_dim,)), ((), ())),
        preferred_element_type=jnp.float32,
    )


def rms_forward(hidden, gain_vector):
    inv_scale = lax.rsqrt(jnp.mean(hidden * hidden, axis=-1, keepdims=True) + norm_eps)
    normed = hidden * inv_scale
    return (normed * gain_vector, normed, inv_scale)


def rms_backward(grad_normed_out, gain_vector, normed, inv_scale):
    grad_scaled = grad_normed_out * gain_vector
    grad_gain = jnp.sum(grad_normed_out * normed, axis=0)
    inner_mean = jnp.mean(grad_scaled * normed, axis=-1, keepdims=True)
    return (inv_scale * (grad_scaled - normed * inner_mean), grad_gain)


def rope_tables(length, head_dim):
    half_dim = head_dim // 2
    frequency = rope_base ** (-(jnp.arange(half_dim, dtype=jnp.float32) * 2.0) / head_dim)
    angles = jnp.arange(length, dtype=jnp.float32)[:, None] * frequency[None, :]
    cosine_table = jnp.concatenate([jnp.cos(angles), jnp.cos(angles)], axis=-1)[:, None, :]
    sine_table = jnp.concatenate([jnp.sin(angles), jnp.sin(angles)], axis=-1)[:, None, :]
    return (cosine_table, sine_table)


def rotate_forward(values, cosine_table, sine_table):
    half_dim = values.shape[-1] // 2
    turned = jnp.concatenate([-values[..., half_dim:], values[..., :half_dim]], axis=-1)
    return values * cosine_table + turned * sine_table


def rotate_backward(grad_rows, cosine_table, sine_table):
    half_dim = grad_rows.shape[-1] // 2
    scaled = grad_rows * sine_table
    turned = jnp.concatenate([scaled[..., half_dim:], -scaled[..., :half_dim]], axis=-1)
    return grad_rows * cosine_table + turned


def gated_backward(grad_act, gate_up):
    sigmoid_gate = jax.nn.sigmoid(gate_up[0])
    grad_gate = grad_act * gate_up[1] * sigmoid_gate * (1.0 + gate_up[0] * (1.0 - sigmoid_gate))
    grad_up = grad_act * gate_up[0] * sigmoid_gate
    return jnp.stack([grad_gate, grad_up]).astype(jnp.bfloat16)


def slot_table(routes, experts, capacity):
    pair_experts = routes.reshape(-1)
    choose = (pair_experts[:, None] == jnp.arange(experts, dtype=jnp.int32)[None, :]).astype(
        jnp.int32
    )
    before = jnp.cumsum(choose, axis=0) - choose
    slot_number = jnp.sum(before * choose, axis=1)
    slot_dest = pair_experts * capacity + slot_number
    pair_count = pair_experts.shape[0]
    slot_owner = (
        jnp.full((experts * capacity,), pair_count, jnp.int32)
        .at[slot_dest]
        .set(jnp.arange(pair_count, dtype=jnp.int32))
    )
    return (slot_dest, slot_owner)


def routed_device(
    tokens,
    norm1_gain,
    w_qkv,
    b_qkv,
    w_out,
    norm2_gain,
    w_router,
    w_sgate,
    w_shared_gu,
    w_shared_down,
    w_expert_gu,
    w_expert_down,
    routes,
    grad_out,
):
    seq_rows, features = tokens.shape
    top_count = routes.shape[1]
    expert_count = w_router.shape[1]
    heads_here = b_qkv.shape[1]
    head_dim = b_qkv.shape[2]
    lane_count = lax.axis_size("tp")
    lane_index = lax.axis_index("tp")
    capacity = lane_count * (5 * seq_rows * top_count // (4 * expert_count * lane_count))
    out_rows = seq_rows // lane_count
    row_start = lane_index * out_rows
    score_scale = head_dim ** (-0.5)
    residual = tokens.astype(jnp.float32)
    normed_one, unit_one, scale_one = rms_forward(residual, norm1_gain)
    low_one = normed_one.astype(jnp.bfloat16)
    qkv_pre = jnp.einsum("ld,cde->cle", low_one, w_qkv, preferred_element_type=jnp.float32)
    qkv_pre = qkv_pre + b_qkv.reshape(3, 1, -1).astype(jnp.float32)
    cosine_table, sine_table = rope_tables(seq_rows, head_dim)
    shaped = qkv_pre.reshape(3, seq_rows, heads_here, head_dim)
    queries = rotate_forward(shaped[0], cosine_table, sine_table).astype(jnp.bfloat16)
    key_rows = rotate_forward(shaped[1], cosine_table, sine_table).astype(jnp.bfloat16)
    value_rows = shaped[2].astype(jnp.bfloat16)
    positions = jnp.arange(seq_rows)
    causal = positions[None, :] <= positions[:, None]

    def attn_scores():
        raw_scores = (
            jnp.einsum("qhd,khd->hqk", queries, key_rows, preferred_element_type=jnp.float32)
            * score_scale
        )
        return jnp.where(causal[None], raw_scores, masked_score)

    scores = attn_scores()
    score_peak = jnp.max(scores, axis=-1, keepdims=True)
    log_total = score_peak + jnp.log(jnp.sum(jnp.exp(scores - score_peak), axis=-1, keepdims=True))
    attn_probs = jnp.exp(scores - log_total).astype(jnp.bfloat16)
    attn_mixed = jnp.einsum(
        "hqk,khd->qhd", attn_probs, value_rows, preferred_element_type=jnp.float32
    )
    attn_mixed = attn_mixed.reshape(seq_rows, -1).astype(jnp.bfloat16)
    attn_total = lax.psum(jnp.dot(attn_mixed, w_out, preferred_element_type=jnp.float32), "tp")
    hidden = residual + attn_total
    normed_two, unit_two, scale_two = rms_forward(hidden, norm2_gain)
    low_two = normed_two.astype(jnp.bfloat16)
    router_probs = jax.nn.softmax(
        jnp.dot(low_two, w_router, preferred_element_type=jnp.float32), axis=-1
    )
    route_hits = (
        routes[:, :, None] == jnp.arange(expert_count, dtype=jnp.int32)[None, None, :]
    ).astype(jnp.float32)
    gate_values = jnp.sum(router_probs[:, None, :] * route_hits, axis=-1)
    shared_gate = jax.nn.sigmoid(jnp.dot(low_two, w_sgate, preferred_element_type=jnp.float32))
    shared_gu = jnp.einsum("ld,cdf->clf", low_two, w_shared_gu, preferred_element_type=jnp.float32)
    shared_act = (jax.nn.silu(shared_gu[0]) * shared_gu[1]).astype(jnp.bfloat16)
    shared_part = jnp.dot(shared_act, w_shared_down, preferred_element_type=jnp.float32)
    slot_dest, slot_owner = slot_table(routes, expert_count, capacity)
    slot_source = (slot_owner // top_count).reshape(expert_count, capacity)
    owner_table = slot_owner.reshape(expert_count, capacity)
    padded_two = jnp.concatenate([low_two, jnp.zeros((1, features), jnp.bfloat16)], axis=0)
    arrived = lax.all_to_all(padded_two[slot_source], "ep", split_axis=0, concat_axis=0, tiled=True)
    expert_in = arrived.reshape(-1, features)
    gate_up_weight = w_expert_gu[0]
    down_weight = w_expert_down[0]
    gate_up = jnp.einsum(
        "rd,cdf->crf", expert_in, gate_up_weight, preferred_element_type=jnp.float32
    )
    expert_act = (jax.nn.silu(gate_up[0]) * gate_up[1]).astype(jnp.bfloat16)
    expert_part = jnp.dot(expert_act, down_weight, preferred_element_type=jnp.float32).astype(
        jnp.bfloat16
    )
    expert_part = expert_part.reshape(expert_count, capacity, features)
    returned = lax.all_to_all(expert_part, "ep", split_axis=0, concat_axis=0, tiled=True)
    return_table = returned.reshape(-1, features)
    return_table = jnp.concatenate(
        [return_table, jnp.zeros((1, features), return_table.dtype)], axis=0
    )
    picked = return_table[slot_dest].reshape(seq_rows, top_count, features)
    expert_sum = jnp.zeros((seq_rows, features), jnp.float32)
    for route_slot in range(top_count):
        expert_sum = expert_sum + gate_values[:, route_slot, None] * picked[:, route_slot].astype(
            jnp.float32
        )
    mlp_total = lax.psum(
        (shared_gate[:, None] * shared_part + expert_sum).astype(jnp.bfloat16), "tp"
    ).astype(jnp.float32)
    output = hidden + mlp_total
    output_rows = lax.dynamic_slice_in_dim(output, row_start, out_rows, 0).astype(jnp.bfloat16)
    grad_output = grad_out.astype(jnp.float32)
    grad_sout = (shared_gate[:, None] * grad_output).astype(jnp.bfloat16)
    grad_shared_down = contract(shared_act, grad_sout, 0, 0)
    grad_sgu = gated_backward(contract(grad_sout, w_shared_down, 1, 1), shared_gu)
    grad_shared_gu = jnp.einsum(
        "ld,clf->cdf", low_two, grad_sgu, preferred_element_type=jnp.float32
    )
    grad_low_two = jnp.einsum(
        "clf,cdf->ld", grad_sgu, w_shared_gu, preferred_element_type=jnp.float32
    )
    shared_dot = jnp.sum(grad_output * shared_part, axis=-1)
    gate_dot = jnp.sum(grad_output[:, None, :] * picked.astype(jnp.float32), axis=-1)
    gate_flat = jnp.concatenate([gate_values.reshape(-1), jnp.zeros((1,), jnp.float32)])
    padded_grad = jnp.concatenate([grad_output, jnp.zeros((1, features), jnp.float32)], axis=0)
    sent_grads = (padded_grad[slot_source] * gate_flat[owner_table][:, :, None]).astype(
        jnp.bfloat16
    )
    grad_arrived = lax.all_to_all(sent_grads, "ep", split_axis=0, concat_axis=0, tiled=True)
    grad_arrived = grad_arrived.reshape(-1, features)
    grad_expert_down = contract(expert_act, grad_arrived, 0, 0)
    grad_egu = gated_backward(contract(grad_arrived, down_weight, 1, 1), gate_up)
    grad_expert_gu = jnp.einsum(
        "rd,crf->cdf", expert_in, grad_egu, preferred_element_type=jnp.float32
    )
    grad_sent = jnp.einsum(
        "crf,cdf->rd", grad_egu, gate_up_weight, preferred_element_type=jnp.float32
    ).astype(jnp.bfloat16)
    grad_returned = lax.all_to_all(
        grad_sent.reshape(expert_count, capacity, features),
        "ep",
        split_axis=0,
        concat_axis=0,
        tiled=True,
    )
    grad_pairs = grad_returned.reshape(-1, features)[slot_dest].reshape(
        seq_rows, top_count, features
    )
    grad_low_two = grad_low_two + jnp.sum(grad_pairs.astype(jnp.float32), axis=1)
    grad_low_two, gate_dot, shared_dot = (
        lax.psum(grad_low_two.astype(jnp.bfloat16), "tp").astype(jnp.float32),
        lax.psum(gate_dot.astype(jnp.bfloat16), "tp").astype(jnp.float32),
        lax.psum(shared_dot.astype(jnp.bfloat16), "tp").astype(jnp.float32),
    )
    grad_sgate_logit = (shared_dot * shared_gate * (1.0 - shared_gate)).astype(jnp.bfloat16)
    grad_sgate = contract(low_two, grad_sgate_logit, 0, 0)
    grad_probs = jnp.sum(gate_dot[:, :, None] * route_hits, axis=1)
    grad_logits = router_probs * (
        grad_probs - jnp.sum(router_probs * grad_probs, axis=-1, keepdims=True)
    )
    grad_logits = grad_logits.astype(jnp.bfloat16)
    grad_router = contract(low_two, grad_logits, 0, 0)
    grad_low_two = (
        grad_low_two
        + grad_sgate_logit.astype(jnp.float32)[:, None] * w_sgate.astype(jnp.float32)[None, :]
    )
    grad_low_two = grad_low_two + contract(grad_logits, w_router, 1, 1)
    grad_hidden_norm, grad_norm_two = rms_backward(grad_low_two, norm2_gain, unit_two, scale_two)
    grad_hidden = grad_output + grad_hidden_norm
    grad_attn = grad_hidden.astype(jnp.bfloat16)
    grad_out_weight = contract(attn_mixed, grad_attn, 0, 0)
    grad_mixed = (
        contract(grad_attn, w_out, 1, 1)
        .astype(jnp.bfloat16)
        .reshape(seq_rows, heads_here, head_dim)
    )
    again_probs = jnp.exp(attn_scores() - log_total)
    grad_values = jnp.einsum(
        "hqk,qhd->khd",
        again_probs.astype(jnp.bfloat16),
        grad_mixed,
        preferred_element_type=jnp.float32,
    )
    grad_probs_attn = jnp.einsum(
        "qhd,khd->hqk", grad_mixed, value_rows, preferred_element_type=jnp.float32
    )
    grad_scores = again_probs * (
        grad_probs_attn - jnp.sum(again_probs * grad_probs_attn, axis=-1, keepdims=True)
    )
    grad_scores = grad_scores.astype(jnp.bfloat16)
    grad_queries = (
        jnp.einsum("hqk,khd->qhd", grad_scores, key_rows, preferred_element_type=jnp.float32)
        * score_scale
    )
    grad_keys = (
        jnp.einsum("hqk,qhd->khd", grad_scores, queries, preferred_element_type=jnp.float32)
        * score_scale
    )
    grad_pre = jnp.stack(
        [
            rotate_backward(grad_queries, cosine_table, sine_table),
            rotate_backward(grad_keys, cosine_table, sine_table),
            grad_values,
        ]
    )
    grad_pre = grad_pre.reshape(3, seq_rows, -1).astype(jnp.bfloat16)
    grad_bias = jnp.sum(grad_pre.astype(jnp.float32), axis=1).reshape(3, heads_here, head_dim)
    grad_qkv = jnp.einsum("ld,cle->cde", low_one, grad_pre, preferred_element_type=jnp.float32)
    grad_low_one = lax.psum(
        jnp.einsum("cle,cde->ld", grad_pre, w_qkv, preferred_element_type=jnp.float32).astype(
            jnp.bfloat16
        ),
        "tp",
    ).astype(jnp.float32)
    grad_input_norm, grad_norm_one = rms_backward(grad_low_one, norm1_gain, unit_one, scale_one)
    grad_tokens = lax.dynamic_slice_in_dim(grad_hidden + grad_input_norm, row_start, out_rows, 0)
    summed = (
        lax.psum_scatter(grad_norm_one, "ep", scatter_dimension=0, tiled=True),
        lax.psum_scatter(grad_qkv, "ep", scatter_dimension=1, tiled=True),
        lax.psum_scatter(grad_bias, "ep", scatter_dimension=2, tiled=True),
        lax.psum_scatter(grad_out_weight, "ep", scatter_dimension=1, tiled=True),
        lax.psum_scatter(grad_norm_two, "ep", scatter_dimension=0, tiled=True),
        lax.psum_scatter(grad_router, "ep", scatter_dimension=0, tiled=True),
        lax.psum_scatter(grad_sgate, "ep", scatter_dimension=0, tiled=True),
        lax.psum_scatter(grad_shared_gu, "ep", scatter_dimension=1, tiled=True),
        lax.psum_scatter(grad_shared_down, "ep", scatter_dimension=1, tiled=True),
    )
    return (
        output_rows,
        grad_tokens,
        summed[0],
        summed[1],
        summed[2],
        summed[3],
        summed[4],
        summed[5],
        summed[6],
        summed[7],
        summed[8],
        grad_expert_gu[None],
        grad_expert_down[None],
    )


def expert_weights(w_expert_gu, w_expert_down, w_shared_gu, w_shared_down, w_router, w_sgate):
    features, experts = w_router.shape
    groups = lax.axis_size("ep")
    expert_units = w_expert_gu.shape[3]
    share = w_shared_gu.shape[2] // groups
    units = expert_units + share
    padded = -(-(units + experts + 1) // 128) * 128
    start = lax.axis_index("ep") * share
    shared_gu = lax.dynamic_slice_in_dim(w_shared_gu, start, share, 2)
    shared_down = lax.dynamic_slice_in_dim(w_shared_down, start, share, 0)
    gate_side = jnp.concatenate(
        [
            w_expert_gu[0, 0],
            shared_gu[0],
            jnp.zeros((features, padded - units - experts - 1), jnp.bfloat16),
            w_router,
            w_sgate[:, None],
        ],
        axis=1,
    )
    up_side = jnp.concatenate(
        [w_expert_gu[0, 1], shared_gu[1], jnp.zeros((features, padded - units), jnp.bfloat16)],
        axis=1,
    )
    down = jnp.concatenate(
        [w_expert_down[0], shared_down, jnp.zeros((padded - units, features), jnp.bfloat16)], axis=0
    )
    return gate_side, up_side, down, units


def expert_kernel(
    experts,
    expert_units,
    units,
    index_ref,
    rows_ref,
    grads_ref,
    chosen_ref,
    gate_ref,
    up_ref,
    down_ref,
    out_ref,
    back_ref,
    act_ref,
    grad_gate_ref,
    grad_up_ref,
):
    features = rows_ref.shape[1]
    padded = gate_ref.shape[1]
    expert = index_ref[0]
    rows = rows_ref[...]
    gate_pre = jnp.dot(rows, gate_ref[...], preferred_element_type=jnp.float32)
    up_pre = jnp.dot(rows, up_ref[...], preferred_element_type=jnp.float32)
    grad_down_act = contract(grads_ref[...], down_ref[...], 1, 1)
    last = gate_pre[:, padded - 128 :]
    lane = lax.broadcasted_iota(jnp.int32, last.shape, 1)
    first = 127 - experts
    routing = (lane >= first) & (lane < 127)
    peak = jnp.max(jnp.where(routing, last, masked_score), axis=1, keepdims=True)
    powers = jnp.where(routing, jnp.exp(last - peak), 0.0)
    powers = jnp.where(routing, powers, 0.0)
    own_power = jnp.sum(jnp.where(lane == first + expert, powers, 0.0), axis=1, keepdims=True)
    expert_gate = chosen_ref[...] * own_power / jnp.sum(powers, axis=1, keepdims=True)
    token_sgate = jax.nn.sigmoid(
        jnp.sum(jnp.where(lane == 127, last, 0.0), axis=1, keepdims=True)
    )
    column = lax.broadcasted_iota(jnp.int32, gate_pre.shape, 1)
    unit_gate = jnp.where(
        column < expert_units, expert_gate, jnp.where(column < units, token_sgate, 0.0)
    )
    sigmoid_gate = jax.nn.sigmoid(gate_pre)
    silu_gate = gate_pre * sigmoid_gate
    act = silu_gate * up_pre
    gated_act = (act * unit_gate).astype(jnp.bfloat16)
    act_ref[...] = gated_act
    dots = act * grad_down_act
    expert_dot = jnp.sum(jnp.where(column < expert_units, dots, 0.0), axis=1, keepdims=True)
    shared_dot = jnp.sum(
        jnp.where((column >= expert_units) & (column < units), dots, 0.0), axis=1, keepdims=True
    )
    grad_act = grad_down_act * unit_gate
    grad_gate = (
        grad_act * up_pre * sigmoid_gate * (1.0 + gate_pre * (1.0 - sigmoid_gate))
    ).astype(jnp.bfloat16)
    grad_up = (grad_act * silu_gate).astype(jnp.bfloat16)
    grad_gate_ref[...] = grad_gate
    grad_up_ref[...] = grad_up
    piece = 512 if features % 512 == 0 else features
    for start in range(0, features, piece):
        columns = pl.ds(start, piece)
        back_ref[:, columns] = (
            contract(grad_gate, gate_ref[columns, :], 1, 1)
            + contract(grad_up, up_ref[columns, :], 1, 1)
        ).astype(jnp.bfloat16)
        out_ref[:, columns] = jnp.dot(
            gated_act, down_ref[:, columns], preferred_element_type=jnp.float32
        ).astype(jnp.bfloat16)
    back_ref[:, features:] = jnp.where(
        lane == expert, expert_dot, jnp.where(lane == experts, shared_dot, 0.0)
    ).astype(jnp.bfloat16)


def expert_layer(rows, grads, chosen, gate_side, up_side, down, experts, expert_units, units):
    count, features = rows.shape
    padded = down.shape[0]
    block = max(size for size in range(16, 513, 16) if count % size == 0)
    index = lax.axis_index("ep").reshape(1).astype(jnp.int32)

    def moving(width):
        return pl.BlockSpec((block, width), lambda i: (i, 0))

    def held(array):
        return pl.BlockSpec(array.shape, lambda i: (0, 0), pipeline_mode=pl.Buffered(1))

    return pl.pallas_call(
        functools.partial(expert_kernel, experts, expert_units, units),
        grid=(count // block,),
        in_specs=[
            pl.BlockSpec(memory_space=pltpu.SMEM),
            moving(features),
            moving(features),
            moving(1),
            held(gate_side),
            held(up_side),
            held(down),
        ],
        out_specs=[
            moving(features),
            moving(features + 128),
            moving(padded),
            moving(padded),
            moving(padded),
        ],
        out_shape=[
            jax.ShapeDtypeStruct((count, features), jnp.bfloat16),
            jax.ShapeDtypeStruct((count, features + 128), jnp.bfloat16),
            jax.ShapeDtypeStruct((count, padded), jnp.bfloat16),
            jax.ShapeDtypeStruct((count, padded), jnp.bfloat16),
            jax.ShapeDtypeStruct((count, padded), jnp.bfloat16),
        ],
        compiler_params=pltpu.CompilerParams(vmem_limit_bytes=60 * 1024 * 1024),
        cost_estimate=pl.CostEstimate(
            flops=12 * count * features * padded,
            bytes_accessed=8 * count * features,
            transcendentals=count * padded,
        ),
    )(index, rows, grads, chosen, gate_side, up_side, down)


def dense_device(
    tokens,
    norm1_gain,
    w_qkv,
    b_qkv,
    w_out,
    norm2_gain,
    w_router,
    w_sgate,
    w_shared_gu,
    w_shared_down,
    w_expert_gu,
    w_expert_down,
    routes,
    grad_out,
):
    seq_rows, features = tokens.shape
    experts = w_router.shape[1]
    heads_here = b_qkv.shape[1]
    head_dim = b_qkv.shape[2]
    groups = lax.axis_size("ep")
    lanes = lax.axis_size("tp")
    group_index = lax.axis_index("ep")
    lane_index = lax.axis_index("tp")
    own_rows = seq_rows // lanes
    row_start = lane_index * own_rows
    score_scale = head_dim ** (-0.5)

    halves = 2
    half_rows = own_rows // halves

    def mine(array):
        return lax.dynamic_slice_in_dim(array, row_start, own_rows, 0)

    def part_of(array, half):
        cut = array.reshape((lanes, halves, half_rows) + array.shape[1:])[:, half]
        return cut.reshape((lanes * half_rows,) + array.shape[1:])

    all_grads = [
        lax.all_gather(part_of(grad_out, half), "ep", axis=0, tiled=True) for half in range(halves)
    ]
    all_routes = lax.all_gather(routes, "ep", axis=0, tiled=True)
    chosen = jnp.sum((all_routes == group_index).astype(jnp.float32), axis=1, keepdims=True)
    chosen = chosen.reshape(groups, lanes, halves, half_rows)

    residual = tokens.astype(jnp.float32)
    normed_one, unit_one, scale_one = rms_forward(residual, norm1_gain)
    low_one = normed_one.astype(jnp.bfloat16)
    qkv_pre = jnp.einsum("ld,cde->cle", low_one, w_qkv, preferred_element_type=jnp.float32)
    qkv_pre = qkv_pre + b_qkv.reshape(3, 1, -1).astype(jnp.float32)
    cosine_table, sine_table = rope_tables(seq_rows, head_dim)
    shaped = qkv_pre.reshape(3, seq_rows, heads_here, head_dim)
    queries = rotate_forward(shaped[0], cosine_table, sine_table).astype(jnp.bfloat16)
    key_rows = rotate_forward(shaped[1], cosine_table, sine_table).astype(jnp.bfloat16)
    value_rows = shaped[2].astype(jnp.bfloat16)
    positions = jnp.arange(seq_rows)
    causal = positions[None, :] <= positions[:, None]

    def attn_scores():
        raw_scores = (
            jnp.einsum("qhd,khd->hqk", queries, key_rows, preferred_element_type=jnp.float32)
            * score_scale
        )
        return jnp.where(causal[None], raw_scores, masked_score)

    scores = attn_scores()
    score_peak = jnp.max(scores, axis=-1, keepdims=True)
    log_total = score_peak + jnp.log(jnp.sum(jnp.exp(scores - score_peak), axis=-1, keepdims=True))
    attn_probs = jnp.exp(scores - log_total).astype(jnp.bfloat16)
    attn_mixed = jnp.einsum(
        "hqk,khd->qhd", attn_probs, value_rows, preferred_element_type=jnp.float32
    )
    attn_mixed = attn_mixed.reshape(seq_rows, -1).astype(jnp.bfloat16)
    attn_part = jnp.dot(attn_mixed, w_out, preferred_element_type=jnp.float32)
    attn_part = attn_part.astype(jnp.bfloat16)
    gate_side, up_side, down, units = expert_weights(
        w_expert_gu, w_expert_down, w_shared_gu, w_shared_down, w_router, w_sgate
    )
    expert_units = w_expert_gu.shape[3]
    own_tokens = mine(tokens)
    own_grads = mine(grad_out).astype(jnp.float32)
    own_hits = jnp.sum(
        (mine(routes)[:, :, None] == jnp.arange(experts, dtype=jnp.int32)[None, None, :]).astype(
            jnp.float32
        ),
        axis=1,
    )

    rows_of, kept, layer = [], [], []
    for half in range(halves):
        here = slice(half * half_rows, (half + 1) * half_rows)
        attn_total = lax.psum_scatter(
            part_of(attn_part, half), "tp", scatter_dimension=0, tiled=True
        )
        hidden = own_tokens[here].astype(jnp.float32) + attn_total.astype(jnp.float32)
        normed_two, unit_two, scale_two = rms_forward(hidden, norm2_gain)
        low_two = normed_two.astype(jnp.bfloat16)
        rows_of.append(lax.all_gather(low_two, ("ep", "tp"), axis=0, tiled=True))
        kept.append((hidden, unit_two, scale_two, low_two))
    for half in range(halves):
        layer.append(
            expert_layer(
                rows_of[half],
                all_grads[half],
                chosen[:, :, half].reshape(-1, 1),
                gate_side,
                up_side,
                down,
                experts,
                expert_units,
                units,
            )
        )

    grad_hidden, gathered, small_sums, back_sums = [], [], [], []
    for half in range(halves):
        here = slice(half * half_rows, (half + 1) * half_rows)
        hidden, unit_two, scale_two, low_two = kept[half]
        grad_sum = lax.psum_scatter(layer[half][1], "ep", scatter_dimension=0, tiled=True)
        back_sums.append(grad_sum)
        grad_sum = lax.psum_scatter(grad_sum, "tp", scatter_dimension=0, tiled=True)
        grad_sum = grad_sum.astype(jnp.float32)
        router_probs = jax.nn.softmax(
            jnp.dot(low_two, w_router, preferred_element_type=jnp.float32), axis=-1
        )
        shared_gate = jax.nn.sigmoid(
            jnp.dot(low_two, w_sgate, preferred_element_type=jnp.float32)
        )
        grad_probs = grad_sum[:, features : features + experts] * own_hits[here]
        own_sdot = grad_sum[:, features + experts]
        grad_sgate_logit = (own_sdot * shared_gate * (1.0 - shared_gate)).astype(jnp.bfloat16)
        grad_logits = router_probs * (
            grad_probs - jnp.sum(router_probs * grad_probs, axis=-1, keepdims=True)
        )
        grad_logits = grad_logits.astype(jnp.bfloat16)
        grad_low_two = (
            grad_sum[:, :features]
            + grad_sgate_logit.astype(jnp.float32)[:, None] * w_sgate.astype(jnp.float32)[None, :]
            + contract(grad_logits, w_router, 1, 1)
        )
        grad_hidden_norm, grad_norm_two = rms_backward(
            grad_low_two, norm2_gain, unit_two, scale_two
        )
        grad_hidden.append(own_grads[here] + grad_hidden_norm)
        gathered.append(
            lax.all_gather(grad_hidden[half].astype(jnp.bfloat16), "tp", axis=0, tiled=True)
        )
        grad_router = contract(low_two, grad_logits, 0, 0)
        grad_sgate = contract(low_two, grad_sgate_logit, 0, 0)
        small_sums.append(
            jnp.concatenate([grad_norm_two[None], grad_sgate[None], grad_router.T], axis=0)
        )
    grad_hidden = jnp.concatenate(grad_hidden, axis=0)
    grad_attn = jnp.stack(
        [piece.reshape(lanes, half_rows, features) for piece in gathered], axis=1
    ).reshape(seq_rows, features)

    output_rows = []
    for half in range(halves):
        out_part, _ = lax.optimization_barrier((layer[half][0], back_sums[-1]))
        out_sum = lax.psum_scatter(out_part, "ep", scatter_dimension=0, tiled=True)
        out_sum = lax.psum_scatter(out_sum, "tp", scatter_dimension=0, tiled=True)
        output_rows.append((kept[half][0] + out_sum.astype(jnp.float32)).astype(jnp.bfloat16))
    output_rows = jnp.concatenate(output_rows, axis=0)

    def over_rows(left, right):
        return functools.reduce(
            jnp.add, [contract(left[half], right[half], 0, 0) for half in range(halves)]
        )

    grad_gate_weight = over_rows(rows_of, [results[3] for results in layer])
    grad_up_weight = over_rows(rows_of, [results[4] for results in layer])
    grad_down_weight = over_rows([results[2] for results in layer], all_grads)
    grad_expert_gu = jnp.stack(
        [grad_gate_weight[:, :expert_units], grad_up_weight[:, :expert_units]]
    )
    grad_expert_down = grad_down_weight[:expert_units]
    share = units - expert_units
    sent_shared = jnp.concatenate(
        [
            grad_gate_weight[:, expert_units:units],
            grad_up_weight[:, expert_units:units],
            grad_down_weight[expert_units:units].T,
        ],
        axis=1,
    ).astype(jnp.bfloat16)
    got_shared = lax.all_to_all(
        sent_shared.reshape(groups, features // groups, 3 * share), "ep", 0, 0, tiled=True
    ).astype(jnp.float32)
    got_shared = got_shared.reshape(groups, features // groups, 3, share)
    grad_shared_gu = jnp.transpose(got_shared[:, :, :2], (2, 1, 0, 3)).reshape(
        2, features // groups, groups * share
    )
    grad_shared_down = jnp.transpose(got_shared[:, :, 2], (0, 2, 1)).reshape(
        groups * share, features // groups
    )

    grad_mixed = (
        contract(grad_attn, w_out, 1, 1)
        .astype(jnp.bfloat16)
        .reshape(seq_rows, heads_here, head_dim)
    )
    again_probs = jnp.exp(attn_scores() - log_total)
    grad_values = jnp.einsum(
        "hqk,qhd->khd",
        again_probs.astype(jnp.bfloat16),
        grad_mixed,
        preferred_element_type=jnp.float32,
    )
    grad_probs_attn = jnp.einsum(
        "qhd,khd->hqk", grad_mixed, value_rows, preferred_element_type=jnp.float32
    )
    grad_scores = again_probs * (
        grad_probs_attn - jnp.sum(again_probs * grad_probs_attn, axis=-1, keepdims=True)
    )
    grad_scores = grad_scores.astype(jnp.bfloat16)
    grad_queries = (
        jnp.einsum("hqk,khd->qhd", grad_scores, key_rows, preferred_element_type=jnp.float32)
        * score_scale
    )
    grad_keys = (
        jnp.einsum("hqk,qhd->khd", grad_scores, queries, preferred_element_type=jnp.float32)
        * score_scale
    )
    grad_pre = jnp.stack(
        [
            rotate_backward(grad_queries, cosine_table, sine_table),
            rotate_backward(grad_keys, cosine_table, sine_table),
            grad_values,
        ]
    )
    grad_pre = grad_pre.reshape(3, seq_rows, -1).astype(jnp.bfloat16)
    low_one_part = jnp.einsum("cle,cde->ld", grad_pre, w_qkv, preferred_element_type=jnp.float32)
    grad_norm_one = jnp.sum(low_one_part * unit_one, axis=0)
    grad_low_one = lax.psum_scatter(
        low_one_part.astype(jnp.bfloat16), "tp", scatter_dimension=0, tiled=True
    ).astype(jnp.float32)
    grad_bias = jnp.sum(grad_pre.astype(jnp.float32), axis=1).reshape(3, heads_here, head_dim)
    grad_qkv = jnp.einsum("ld,cle->cde", low_one, grad_pre, preferred_element_type=jnp.float32)
    grad_out_weight = contract(attn_mixed, grad_attn, 0, 0)
    grad_input_norm, _ = rms_backward(grad_low_one, norm1_gain, mine(unit_one), mine(scale_one))
    grad_tokens = grad_hidden + grad_input_norm

    small = jnp.concatenate([grad_norm_one[None], small_sums[0] + small_sums[1]], axis=0)
    small = lax.psum(small.reshape(-1, 128), ("ep", "tp")).reshape(small.shape)
    small = lax.dynamic_slice_in_dim(
        small, group_index * (features // groups), features // groups, 1
    )
    return (
        output_rows,
        grad_tokens,
        small[0],
        lax.psum_scatter(
            grad_qkv.astype(jnp.bfloat16), "ep", scatter_dimension=1, tiled=True
        ).astype(jnp.float32),
        lax.psum_scatter(grad_bias, "ep", scatter_dimension=2, tiled=True),
        lax.psum_scatter(
            grad_out_weight.astype(jnp.bfloat16), "ep", scatter_dimension=1, tiled=True
        ).astype(jnp.float32),
        small[1],
        small[3:].T,
        small[2],
        grad_shared_gu,
        grad_shared_down,
        grad_expert_gu[None],
        grad_expert_down[None],
    )


def per_device(*arrays):
    experts, chosen = arrays[6].shape[1], arrays[12].shape[1]
    if experts <= 2 * chosen:
        return dense_device(*arrays)
    return routed_device(*arrays)


def solution(mesh):
    return jax.shard_map(
        per_device,
        mesh=mesh,
        in_specs=(
            P("ep", None),
            P(),
            P(None, None, "tp"),
            P(None, "tp", None),
            P("tp", None),
            P(),
            P(),
            P(),
            P(None, None, "tp"),
            P("tp", None),
            P("ep", None, None, "tp"),
            P("ep", "tp", None),
            P("ep", None),
            P("ep", None),
        ),
        out_specs=(
            P(("ep", "tp"), None),
            P(("ep", "tp"), None),
            P("ep"),
            P(None, "ep", "tp"),
            P(None, "tp", "ep"),
            P("tp", "ep"),
            P("ep"),
            P("ep", None),
            P("ep"),
            P(None, "ep", "tp"),
            P("tp", "ep"),
            P("ep", None, None, "tp"),
            P("ep", "tp", None),
        ),
        check_vma=False,
    )
```

```python
import functools

import jax
import jax.numpy as jnp
from jax import lax
from jax.experimental import pallas as pl
from jax.experimental.pallas import tpu as pltpu
from jax.sharding import PartitionSpec as P


norm_eps = 1e-06
rope_base = 1000000.0
masked_score = -1e30


def contract(left_side, right_side, left_dim, right_dim):
    return lax.dot_general(
        left_side,
        right_side,
        (((left_dim,), (right_dim,)), ((), ())),
        preferred_element_type=jnp.float32,
    )


def rms_forward(hidden, gain_vector):
    inv_scale = lax.rsqrt(jnp.mean(hidden * hidden, axis=-1, keepdims=True) + norm_eps)
    normed = hidden * inv_scale
    return (normed * gain_vector, normed, inv_scale)


def rms_backward(grad_normed_out, gain_vector, normed, inv_scale):
    grad_scaled = grad_normed_out * gain_vector
    grad_gain = jnp.sum(grad_normed_out * normed, axis=0)
    inner_mean = jnp.mean(grad_scaled * normed, axis=-1, keepdims=True)
    return (inv_scale * (grad_scaled - normed * inner_mean), grad_gain)


def rope_tables(length, head_dim):
    half_dim = head_dim // 2
    frequency = rope_base ** (-(jnp.arange(half_dim, dtype=jnp.float32) * 2.0) / head_dim)
    angles = jnp.arange(length, dtype=jnp.float32)[:, None] * frequency[None, :]
    cosine_table = jnp.concatenate([jnp.cos(angles), jnp.cos(angles)], axis=-1)[:, None, :]
    sine_table = jnp.concatenate([jnp.sin(angles), jnp.sin(angles)], axis=-1)[:, None, :]
    return (cosine_table, sine_table)


def rotate_forward(values, cosine_table, sine_table):
    half_dim = values.shape[-1] // 2
    turned = jnp.concatenate([-values[..., half_dim:], values[..., :half_dim]], axis=-1)
    return values * cosine_table + turned * sine_table


def rotate_backward(grad_rows, cosine_table, sine_table):
    half_dim = grad_rows.shape[-1] // 2
    scaled = grad_rows * sine_table
    turned = jnp.concatenate([scaled[..., half_dim:], -scaled[..., :half_dim]], axis=-1)
    return grad_rows * cosine_table + turned


def gated_backward(grad_act, gate_up):
    sigmoid_gate = jax.nn.sigmoid(gate_up[0])
    grad_gate = grad_act * gate_up[1] * sigmoid_gate * (1.0 + gate_up[0] * (1.0 - sigmoid_gate))
    grad_up = grad_act * gate_up[0] * sigmoid_gate
    return jnp.stack([grad_gate, grad_up]).astype(jnp.bfloat16)


def slot_table(routes, experts, capacity):
    pair_experts = routes.reshape(-1)
    choose = (pair_experts[:, None] == jnp.arange(experts, dtype=jnp.int32)[None, :]).astype(
        jnp.int32
    )
    before = jnp.cumsum(choose, axis=0) - choose
    slot_number = jnp.sum(before * choose, axis=1)
    slot_dest = pair_experts * capacity + slot_number
    pair_count = pair_experts.shape[0]
    slot_owner = (
        jnp.full((experts * capacity,), pair_count, jnp.int32)
        .at[slot_dest]
        .set(jnp.arange(pair_count, dtype=jnp.int32))
    )
    return (slot_dest, slot_owner)


def routed_device(
    tokens,
    norm1_gain,
    w_qkv,
    b_qkv,
    w_out,
    norm2_gain,
    w_router,
    w_sgate,
    w_shared_gu,
    w_shared_down,
    w_expert_gu,
    w_expert_down,
    routes,
    grad_out,
):
    seq_rows, features = tokens.shape
    top_count = routes.shape[1]
    expert_count = w_router.shape[1]
    heads_here = b_qkv.shape[1]
    head_dim = b_qkv.shape[2]
    lane_count = lax.axis_size("tp")
    lane_index = lax.axis_index("tp")
    capacity = lane_count * (5 * seq_rows * top_count // (4 * expert_count * lane_count))
    out_rows = seq_rows // lane_count
    row_start = lane_index * out_rows
    score_scale = head_dim ** (-0.5)
    residual = tokens.astype(jnp.float32)
    normed_one, unit_one, scale_one = rms_forward(residual, norm1_gain)
    low_one = normed_one.astype(jnp.bfloat16)
    qkv_pre = jnp.einsum("ld,cde->cle", low_one, w_qkv, preferred_element_type=jnp.float32)
    qkv_pre = qkv_pre + b_qkv.reshape(3, 1, -1).astype(jnp.float32)
    cosine_table, sine_table = rope_tables(seq_rows, head_dim)
    shaped = qkv_pre.reshape(3, seq_rows, heads_here, head_dim)
    queries = rotate_forward(shaped[0], cosine_table, sine_table).astype(jnp.bfloat16)
    key_rows = rotate_forward(shaped[1], cosine_table, sine_table).astype(jnp.bfloat16)
    value_rows = shaped[2].astype(jnp.bfloat16)
    positions = jnp.arange(seq_rows)
    causal = positions[None, :] <= positions[:, None]

    def attn_scores():
        raw_scores = (
            jnp.einsum("qhd,khd->hqk", queries, key_rows, preferred_element_type=jnp.float32)
            * score_scale
        )
        return jnp.where(causal[None], raw_scores, masked_score)

    scores = attn_scores()
    score_peak = jnp.max(scores, axis=-1, keepdims=True)
    log_total = score_peak + jnp.log(jnp.sum(jnp.exp(scores - score_peak), axis=-1, keepdims=True))
    attn_probs = jnp.exp(scores - log_total).astype(jnp.bfloat16)
    attn_mixed = jnp.einsum(
        "hqk,khd->qhd", attn_probs, value_rows, preferred_element_type=jnp.float32
    )
    attn_mixed = attn_mixed.reshape(seq_rows, -1).astype(jnp.bfloat16)
    attn_total = lax.psum(jnp.dot(attn_mixed, w_out, preferred_element_type=jnp.float32), "tp")
    hidden = residual + attn_total
    normed_two, unit_two, scale_two = rms_forward(hidden, norm2_gain)
    low_two = normed_two.astype(jnp.bfloat16)
    router_probs = jax.nn.softmax(
        jnp.dot(low_two, w_router, preferred_element_type=jnp.float32), axis=-1
    )
    route_hits = (
        routes[:, :, None] == jnp.arange(expert_count, dtype=jnp.int32)[None, None, :]
    ).astype(jnp.float32)
    gate_values = jnp.sum(router_probs[:, None, :] * route_hits, axis=-1)
    shared_gate = jax.nn.sigmoid(jnp.dot(low_two, w_sgate, preferred_element_type=jnp.float32))
    shared_gu = jnp.einsum("ld,cdf->clf", low_two, w_shared_gu, preferred_element_type=jnp.float32)
    shared_act = (jax.nn.silu(shared_gu[0]) * shared_gu[1]).astype(jnp.bfloat16)
    shared_part = jnp.dot(shared_act, w_shared_down, preferred_element_type=jnp.float32)
    slot_dest, slot_owner = slot_table(routes, expert_count, capacity)
    slot_source = (slot_owner // top_count).reshape(expert_count, capacity)
    owner_table = slot_owner.reshape(expert_count, capacity)
    padded_two = jnp.concatenate([low_two, jnp.zeros((1, features), jnp.bfloat16)], axis=0)
    arrived = lax.all_to_all(padded_two[slot_source], "ep", split_axis=0, concat_axis=0, tiled=True)
    expert_in = arrived.reshape(-1, features)
    gate_up_weight = w_expert_gu[0]
    down_weight = w_expert_down[0]
    gate_up = jnp.einsum(
        "rd,cdf->crf", expert_in, gate_up_weight, preferred_element_type=jnp.float32
    )
    expert_act = (jax.nn.silu(gate_up[0]) * gate_up[1]).astype(jnp.bfloat16)
    expert_part = jnp.dot(expert_act, down_weight, preferred_element_type=jnp.float32).astype(
        jnp.bfloat16
    )
    expert_part = expert_part.reshape(expert_count, capacity, features)
    returned = lax.all_to_all(expert_part, "ep", split_axis=0, concat_axis=0, tiled=True)
    return_table = returned.reshape(-1, features)
    return_table = jnp.concatenate(
        [return_table, jnp.zeros((1, features), return_table.dtype)], axis=0
    )
    picked = return_table[slot_dest].reshape(seq_rows, top_count, features)
    expert_sum = jnp.zeros((seq_rows, features), jnp.float32)
    for route_slot in range(top_count):
        expert_sum = expert_sum + gate_values[:, route_slot, None] * picked[:, route_slot].astype(
            jnp.float32
        )
    mlp_total = lax.psum(
        (shared_gate[:, None] * shared_part + expert_sum).astype(jnp.bfloat16), "tp"
    ).astype(jnp.float32)
    output = hidden + mlp_total
    output_rows = lax.dynamic_slice_in_dim(output, row_start, out_rows, 0).astype(jnp.bfloat16)
    grad_output = grad_out.astype(jnp.float32)
    grad_sout = (shared_gate[:, None] * grad_output).astype(jnp.bfloat16)
    grad_shared_down = contract(shared_act, grad_sout, 0, 0)
    grad_sgu = gated_backward(contract(grad_sout, w_shared_down, 1, 1), shared_gu)
    grad_shared_gu = jnp.einsum(
        "ld,clf->cdf", low_two, grad_sgu, preferred_element_type=jnp.float32
    )
    grad_low_two = jnp.einsum(
        "clf,cdf->ld", grad_sgu, w_shared_gu, preferred_element_type=jnp.float32
    )
    shared_dot = jnp.sum(grad_output * shared_part, axis=-1)
    gate_dot = jnp.sum(grad_output[:, None, :] * picked.astype(jnp.float32), axis=-1)
    gate_flat = jnp.concatenate([gate_values.reshape(-1), jnp.zeros((1,), jnp.float32)])
    padded_grad = jnp.concatenate([grad_output, jnp.zeros((1, features), jnp.float32)], axis=0)
    sent_grads = (padded_grad[slot_source] * gate_flat[owner_table][:, :, None]).astype(
        jnp.bfloat16
    )
    grad_arrived = lax.all_to_all(sent_grads, "ep", split_axis=0, concat_axis=0, tiled=True)
    grad_arrived = grad_arrived.reshape(-1, features)
    grad_expert_down = contract(expert_act, grad_arrived, 0, 0)
    grad_egu = gated_backward(contract(grad_arrived, down_weight, 1, 1), gate_up)
    grad_expert_gu = jnp.einsum(
        "rd,crf->cdf", expert_in, grad_egu, preferred_element_type=jnp.float32
    )
    grad_sent = jnp.einsum(
        "crf,cdf->rd", grad_egu, gate_up_weight, preferred_element_type=jnp.float32
    ).astype(jnp.bfloat16)
    grad_returned = lax.all_to_all(
        grad_sent.reshape(expert_count, capacity, features),
        "ep",
        split_axis=0,
        concat_axis=0,
        tiled=True,
    )
    grad_pairs = grad_returned.reshape(-1, features)[slot_dest].reshape(
        seq_rows, top_count, features
    )
    grad_low_two = grad_low_two + jnp.sum(grad_pairs.astype(jnp.float32), axis=1)
    grad_low_two, gate_dot, shared_dot = (
        lax.psum(grad_low_two.astype(jnp.bfloat16), "tp").astype(jnp.float32),
        lax.psum(gate_dot.astype(jnp.bfloat16), "tp").astype(jnp.float32),
        lax.psum(shared_dot.astype(jnp.bfloat16), "tp").astype(jnp.float32),
    )
    grad_sgate_logit = (shared_dot * shared_gate * (1.0 - shared_gate)).astype(jnp.bfloat16)
    grad_sgate = contract(low_two, grad_sgate_logit, 0, 0)
    grad_probs = jnp.sum(gate_dot[:, :, None] * route_hits, axis=1)
    grad_logits = router_probs * (
        grad_probs - jnp.sum(router_probs * grad_probs, axis=-1, keepdims=True)
    )
    grad_logits = grad_logits.astype(jnp.bfloat16)
    grad_router = contract(low_two, grad_logits, 0, 0)
    grad_low_two = (
        grad_low_two
        + grad_sgate_logit.astype(jnp.float32)[:, None] * w_sgate.astype(jnp.float32)[None, :]
    )
    grad_low_two = grad_low_two + contract(grad_logits, w_router, 1, 1)
    grad_hidden_norm, grad_norm_two = rms_backward(grad_low_two, norm2_gain, unit_two, scale_two)
    grad_hidden = grad_output + grad_hidden_norm
    grad_attn = grad_hidden.astype(jnp.bfloat16)
    grad_out_weight = contract(attn_mixed, grad_attn, 0, 0)
    grad_mixed = (
        contract(grad_attn, w_out, 1, 1)
        .astype(jnp.bfloat16)
        .reshape(seq_rows, heads_here, head_dim)
    )
    again_probs = jnp.exp(attn_scores() - log_total)
    grad_values = jnp.einsum(
        "hqk,qhd->khd",
        again_probs.astype(jnp.bfloat16),
        grad_mixed,
        preferred_element_type=jnp.float32,
    )
    grad_probs_attn = jnp.einsum(
        "qhd,khd->hqk", grad_mixed, value_rows, preferred_element_type=jnp.float32
    )
    grad_scores = again_probs * (
        grad_probs_attn - jnp.sum(again_probs * grad_probs_attn, axis=-1, keepdims=True)
    )
    grad_scores = grad_scores.astype(jnp.bfloat16)
    grad_queries = (
        jnp.einsum("hqk,khd->qhd", grad_scores, key_rows, preferred_element_type=jnp.float32)
        * score_scale
    )
    grad_keys = (
        jnp.einsum("hqk,qhd->khd", grad_scores, queries, preferred_element_type=jnp.float32)
        * score_scale
    )
    grad_pre = jnp.stack(
        [
            rotate_backward(grad_queries, cosine_table, sine_table),
            rotate_backward(grad_keys, cosine_table, sine_table),
            grad_values,
        ]
    )
    grad_pre = grad_pre.reshape(3, seq_rows, -1).astype(jnp.bfloat16)
    grad_bias = jnp.sum(grad_pre.astype(jnp.float32), axis=1).reshape(3, heads_here, head_dim)
    grad_qkv = jnp.einsum("ld,cle->cde", low_one, grad_pre, preferred_element_type=jnp.float32)
    grad_low_one = lax.psum(
        jnp.einsum("cle,cde->ld", grad_pre, w_qkv, preferred_element_type=jnp.float32).astype(
            jnp.bfloat16
        ),
        "tp",
    ).astype(jnp.float32)
    grad_input_norm, grad_norm_one = rms_backward(grad_low_one, norm1_gain, unit_one, scale_one)
    grad_tokens = lax.dynamic_slice_in_dim(grad_hidden + grad_input_norm, row_start, out_rows, 0)
    summed = (
        lax.psum_scatter(grad_norm_one, "ep", scatter_dimension=0, tiled=True),
        lax.psum_scatter(grad_qkv, "ep", scatter_dimension=1, tiled=True),
        lax.psum_scatter(grad_bias, "ep", scatter_dimension=2, tiled=True),
        lax.psum_scatter(grad_out_weight, "ep", scatter_dimension=1, tiled=True),
        lax.psum_scatter(grad_norm_two, "ep", scatter_dimension=0, tiled=True),
        lax.psum_scatter(grad_router, "ep", scatter_dimension=0, tiled=True),
        lax.psum_scatter(grad_sgate, "ep", scatter_dimension=0, tiled=True),
        lax.psum_scatter(grad_shared_gu, "ep", scatter_dimension=1, tiled=True),
        lax.psum_scatter(grad_shared_down, "ep", scatter_dimension=1, tiled=True),
    )
    return (
        output_rows,
        grad_tokens,
        summed[0],
        summed[1],
        summed[2],
        summed[3],
        summed[4],
        summed[5],
        summed[6],
        summed[7],
        summed[8],
        grad_expert_gu[None],
        grad_expert_down[None],
    )


def lane_scatter_sum(part, lanes):
    rows = part.shape[0] // lanes
    lane = lax.axis_index("tp")
    total = lax.dynamic_slice_in_dim(part, lane * rows, rows, 0).astype(jnp.float32)
    arrived = []
    for shift in range(1, lanes):
        block = lax.dynamic_slice_in_dim(part, (lane + shift) % lanes * rows, rows, 0)
        arrived.append(
            lax.ppermute(block, "tp", [(i, (i + shift) % lanes) for i in range(lanes)])
        )
    for block in arrived:
        total = total + block.astype(jnp.float32)
    return total


def lane_gather(rows, lanes):
    lane = lax.axis_index("tp")
    count = rows.shape[0]
    pieces = [rows] + [
        lax.ppermute(rows, "tp", [(i, (i + shift) % lanes) for i in range(lanes)])
        for shift in range(1, lanes)
    ]
    whole = jnp.zeros((lanes * count, rows.shape[1]), rows.dtype)
    for shift, piece in enumerate(pieces):
        whole = lax.dynamic_update_slice_in_dim(
            whole, piece, (lane + lanes - shift) % lanes * count, 0
        )
    return whole


def expert_weights(w_expert_gu, w_expert_down, w_shared_gu, w_shared_down, w_router, w_sgate):
    features, experts = w_router.shape
    groups = lax.axis_size("ep")
    expert_units = w_expert_gu.shape[3]
    share = w_shared_gu.shape[2] // groups
    units = expert_units + share
    padded = -(-(units + experts + 1) // 128) * 128
    start = lax.axis_index("ep") * share
    shared_gu = lax.dynamic_slice_in_dim(w_shared_gu, start, share, 2)
    shared_down = lax.dynamic_slice_in_dim(w_shared_down, start, share, 0)
    sides = jnp.concatenate(
        [
            w_expert_gu[0, 0],
            shared_gu[0],
            jnp.zeros((features, padded - units - experts - 1), jnp.bfloat16),
            w_router,
            w_sgate[:, None],
            w_expert_gu[0, 1],
            shared_gu[1],
            jnp.zeros((features, padded - units), jnp.bfloat16),
        ],
        axis=1,
    )
    down = jnp.concatenate(
        [w_expert_down[0], shared_down, jnp.zeros((padded - units, features), jnp.bfloat16)], axis=0
    )
    return sides, down, units


def expert_kernel(
    experts,
    expert_units,
    units,
    index_ref,
    rows_ref,
    grads_ref,
    sides_ref,
    down_ref,
    out_ref,
    back_ref,
    act_ref,
    grad_sides_ref,
):
    features = rows_ref.shape[1]
    padded = down_ref.shape[0]
    expert = index_ref[0]
    rows = rows_ref[...]
    both_pre = jnp.dot(rows, sides_ref[...], preferred_element_type=jnp.float32)
    gate_pre, up_pre = both_pre[:, :padded], both_pre[:, padded:]
    grad_down_act = contract(grads_ref[:, :features], down_ref[...], 1, 1)
    last = gate_pre[:, padded - 128 :]
    lane = lax.broadcasted_iota(jnp.int32, last.shape, 1)
    first = 127 - experts
    routing = (lane >= first) & (lane < 127)
    peak = jnp.max(jnp.where(routing, last, masked_score), axis=1, keepdims=True)
    powers = jnp.where(routing, jnp.exp(last - peak), 0.0)
    powers = jnp.where(routing, powers, 0.0)
    own_power = jnp.sum(jnp.where(lane == first + expert, powers, 0.0), axis=1, keepdims=True)
    chosen = jnp.sum(
        jnp.where(lane == expert, grads_ref[:, features:].astype(jnp.float32), 0.0),
        axis=1,
        keepdims=True,
    )
    expert_gate = chosen * own_power / jnp.sum(powers, axis=1, keepdims=True)
    token_sgate = jax.nn.sigmoid(
        jnp.sum(jnp.where(lane == 127, last, 0.0), axis=1, keepdims=True)
    )
    column = lax.broadcasted_iota(jnp.int32, gate_pre.shape, 1)
    unit_gate = jnp.where(
        column < expert_units, expert_gate, jnp.where(column < units, token_sgate, 0.0)
    )
    sigmoid_gate = jax.nn.sigmoid(gate_pre)
    silu_gate = gate_pre * sigmoid_gate
    act = silu_gate * up_pre
    gated_act = (act * unit_gate).astype(jnp.bfloat16)
    act_ref[...] = gated_act
    dots = act * grad_down_act
    expert_dot = jnp.sum(jnp.where(column < expert_units, dots, 0.0), axis=1, keepdims=True)
    shared_dot = jnp.sum(
        jnp.where((column >= expert_units) & (column < units), dots, 0.0), axis=1, keepdims=True
    )
    grad_act = grad_down_act * unit_gate
    grad_gate = (
        grad_act * up_pre * sigmoid_gate * (1.0 + gate_pre * (1.0 - sigmoid_gate))
    ).astype(jnp.bfloat16)
    grad_up = (grad_act * silu_gate).astype(jnp.bfloat16)
    grad_sides = jnp.concatenate([grad_gate, grad_up], axis=1)
    grad_sides_ref[...] = grad_sides
    piece = 512 if features % 512 == 0 else features
    for start in range(0, features, piece):
        columns = pl.ds(start, piece)
        back_ref[:, columns] = contract(grad_sides, sides_ref[columns, :], 1, 1).astype(
            jnp.bfloat16
        )
        out_ref[:, columns] = jnp.dot(
            gated_act, down_ref[:, columns], preferred_element_type=jnp.float32
        ).astype(jnp.bfloat16)
    back_ref[:, features:] = jnp.where(
        lane == expert, expert_dot, jnp.where(lane == experts, shared_dot, 0.0)
    ).astype(jnp.bfloat16)


def expert_layer(rows, grads, sides, down, experts, expert_units, units):
    count, features = rows.shape
    padded = down.shape[0]
    block = max(size for size in range(16, 513, 16) if count % size == 0)
    index = lax.axis_index("ep").reshape(1).astype(jnp.int32)

    def moving(width):
        return pl.BlockSpec((block, width), lambda i: (i, 0))

    def held(array):
        return pl.BlockSpec(array.shape, lambda i: (0, 0), pipeline_mode=pl.Buffered(1))

    return pl.pallas_call(
        functools.partial(expert_kernel, experts, expert_units, units),
        grid=(count // block,),
        in_specs=[
            pl.BlockSpec(memory_space=pltpu.SMEM),
            moving(features),
            moving(features + 128),
            held(sides),
            held(down),
        ],
        out_specs=[
            moving(features),
            moving(features + 128),
            moving(padded),
            moving(2 * padded),
        ],
        out_shape=[
            jax.ShapeDtypeStruct((count, features), jnp.bfloat16),
            jax.ShapeDtypeStruct((count, features + 128), jnp.bfloat16),
            jax.ShapeDtypeStruct((count, padded), jnp.bfloat16),
            jax.ShapeDtypeStruct((count, 2 * padded), jnp.bfloat16),
        ],
        compiler_params=pltpu.CompilerParams(vmem_limit_bytes=60 * 1024 * 1024),
        cost_estimate=pl.CostEstimate(
            flops=12 * count * features * padded,
            bytes_accessed=8 * count * features,
            transcendentals=count * padded,
        ),
    )(index, rows, grads, sides, down)


def dense_device(
    tokens,
    norm1_gain,
    w_qkv,
    b_qkv,
    w_out,
    norm2_gain,
    w_router,
    w_sgate,
    w_shared_gu,
    w_shared_down,
    w_expert_gu,
    w_expert_down,
    routes,
    grad_out,
):
    seq_rows, features = tokens.shape
    experts = w_router.shape[1]
    heads_here = b_qkv.shape[1]
    head_dim = b_qkv.shape[2]
    groups = lax.axis_size("ep")
    lanes = lax.axis_size("tp")
    lane_index = lax.axis_index("tp")
    own_rows = seq_rows // lanes
    row_start = lane_index * own_rows
    score_scale = head_dim ** (-0.5)

    halves = 1
    half_rows = own_rows // halves

    def mine(array):
        return lax.dynamic_slice_in_dim(array, row_start, own_rows, 0)

    def part_of(array, half):
        cut = array.reshape((lanes, halves, half_rows) + array.shape[1:])[:, half]
        return cut.reshape((lanes * half_rows,) + array.shape[1:])

    hits = jnp.sum(
        (routes[:, :, None] == jnp.arange(128, dtype=jnp.int32)[None, None, :]).astype(
            jnp.bfloat16
        ),
        axis=1,
    )
    marked_grads = jnp.concatenate([grad_out, hits], axis=1)
    all_grads = [
        lax.all_gather(part_of(marked_grads, half), "ep", axis=0, tiled=True)
        for half in range(halves)
    ]

    residual = tokens.astype(jnp.float32)
    normed_one, unit_one, scale_one = rms_forward(residual, norm1_gain)
    low_one = normed_one.astype(jnp.bfloat16)
    qkv_pre = jnp.einsum("ld,cde->cle", low_one, w_qkv, preferred_element_type=jnp.float32)
    qkv_pre = qkv_pre + b_qkv.reshape(3, 1, -1).astype(jnp.float32)
    cosine_table, sine_table = rope_tables(seq_rows, head_dim)
    shaped = qkv_pre.reshape(3, seq_rows, heads_here, head_dim)
    queries = rotate_forward(shaped[0], cosine_table, sine_table).astype(jnp.bfloat16)
    key_rows = rotate_forward(shaped[1], cosine_table, sine_table).astype(jnp.bfloat16)
    value_rows = shaped[2].astype(jnp.bfloat16)
    positions = jnp.arange(seq_rows)
    causal = positions[None, :] <= positions[:, None]

    def attn_scores():
        raw_scores = (
            jnp.einsum("qhd,khd->hqk", queries, key_rows, preferred_element_type=jnp.float32)
            * score_scale
        )
        return jnp.where(causal[None], raw_scores, masked_score)

    scores = attn_scores()
    score_peak = jnp.max(scores, axis=-1, keepdims=True)
    log_total = score_peak + jnp.log(jnp.sum(jnp.exp(scores - score_peak), axis=-1, keepdims=True))
    attn_probs = jnp.exp(scores - log_total).astype(jnp.bfloat16)
    attn_mixed = jnp.einsum(
        "hqk,khd->qhd", attn_probs, value_rows, preferred_element_type=jnp.float32
    )
    attn_mixed = attn_mixed.reshape(seq_rows, -1).astype(jnp.bfloat16)
    attn_part = jnp.dot(attn_mixed, w_out, preferred_element_type=jnp.float32)
    attn_part = attn_part.astype(jnp.bfloat16)
    sides, down, units = expert_weights(
        w_expert_gu, w_expert_down, w_shared_gu, w_shared_down, w_router, w_sgate
    )
    expert_units = w_expert_gu.shape[3]
    own_tokens = mine(tokens)
    own_grads = mine(grad_out).astype(jnp.float32)
    own_hits = mine(hits)[:, :experts].astype(jnp.float32)

    rows_of, kept, layer = [], [], []
    for half in range(halves):
        here = slice(half * half_rows, (half + 1) * half_rows)
        attn_total = lane_scatter_sum(part_of(attn_part, half), lanes)
        hidden = own_tokens[here].astype(jnp.float32) + attn_total
        normed_two, unit_two, scale_two = rms_forward(hidden, norm2_gain)
        low_two = normed_two.astype(jnp.bfloat16)
        rows_of.append(lax.all_gather(low_two, ("ep", "tp"), axis=0, tiled=True))
        kept.append((hidden, unit_two, scale_two, low_two))
    for half in range(halves):
        layer.append(
            expert_layer(
                rows_of[half],
                all_grads[half],
                sides,
                down,
                experts,
                expert_units,
                units,
            )
        )

    def over_rows(left, right):
        return functools.reduce(
            jnp.add, [contract(left[half], right[half], 0, 0) for half in range(halves)]
        )

    grad_sides = over_rows(rows_of, [results[3] for results in layer])
    grad_down_weight = over_rows([results[2] for results in layer], all_grads)
    grad_down_weight = grad_down_weight[:, :features]
    grad_gate_weight = grad_sides[:, : down.shape[0]]
    grad_up_weight = grad_sides[:, down.shape[0] :]
    grad_expert_gu = jnp.stack(
        [grad_gate_weight[:, :expert_units], grad_up_weight[:, :expert_units]]
    )
    grad_expert_down = grad_down_weight[:expert_units]
    share = units - expert_units
    sent_shared = jnp.concatenate(
        [
            grad_gate_weight[:, expert_units:units],
            grad_up_weight[:, expert_units:units],
            grad_down_weight[expert_units:units].T,
        ],
        axis=1,
    ).astype(jnp.bfloat16)
    grad_hidden, gathered, small_sums, back_sums = [], [], [], []
    for half in range(halves):
        here = slice(half * half_rows, (half + 1) * half_rows)
        hidden, unit_two, scale_two, low_two = kept[half]
        grad_sum = lax.psum_scatter(layer[half][1], "ep", scatter_dimension=0, tiled=True)
        if half == halves - 1:
            grad_sum, sent_shared = lax.optimization_barrier((grad_sum, sent_shared))
        back_sums.append(grad_sum)
        grad_sum = lane_scatter_sum(grad_sum, lanes)
        router_probs = jax.nn.softmax(
            jnp.dot(low_two, w_router, preferred_element_type=jnp.float32), axis=-1
        )
        shared_gate = jax.nn.sigmoid(
            jnp.dot(low_two, w_sgate, preferred_element_type=jnp.float32)
        )
        grad_probs = grad_sum[:, features : features + experts] * own_hits[here]
        own_sdot = grad_sum[:, features + experts]
        grad_sgate_logit = (own_sdot * shared_gate * (1.0 - shared_gate)).astype(jnp.bfloat16)
        grad_logits = router_probs * (
            grad_probs - jnp.sum(router_probs * grad_probs, axis=-1, keepdims=True)
        )
        grad_logits = grad_logits.astype(jnp.bfloat16)
        grad_low_two = (
            grad_sum[:, :features]
            + grad_sgate_logit.astype(jnp.float32)[:, None] * w_sgate.astype(jnp.float32)[None, :]
            + contract(grad_logits, w_router, 1, 1)
        )
        grad_hidden_norm, grad_norm_two = rms_backward(
            grad_low_two, norm2_gain, unit_two, scale_two
        )
        grad_hidden.append(own_grads[here] + grad_hidden_norm)
        gathered.append(lane_gather(grad_hidden[half].astype(jnp.bfloat16), lanes))
        grad_router = contract(low_two, grad_logits, 0, 0)
        grad_sgate = contract(low_two, grad_sgate_logit, 0, 0)
        small_sums.append(
            jnp.concatenate([grad_norm_two[None], grad_sgate[None], grad_router.T], axis=0)
        )
    grad_hidden = jnp.concatenate(grad_hidden, axis=0)
    grad_attn = jnp.stack(
        [piece.reshape(lanes, half_rows, features) for piece in gathered], axis=1
    ).reshape(seq_rows, features)

    output_rows = []
    for half in range(halves):
        out_part, _ = lax.optimization_barrier((layer[half][0], back_sums[-1]))
        out_sum = lax.psum_scatter(out_part, "ep", scatter_dimension=0, tiled=True)
        out_sum = lane_scatter_sum(out_sum, lanes)
        output_rows.append((kept[half][0] + out_sum).astype(jnp.bfloat16))
    output_rows = jnp.concatenate(output_rows, axis=0)

    got_shared = lax.all_to_all(
        sent_shared.reshape(groups, features // groups, 3 * share), "ep", 0, 0, tiled=True
    ).astype(jnp.float32)
    got_shared = got_shared.reshape(groups, features // groups, 3, share)
    got_shared, grad_attn = lax.optimization_barrier((got_shared, grad_attn))
    grad_shared_gu = jnp.transpose(got_shared[:, :, :2], (2, 1, 0, 3)).reshape(
        2, features // groups, groups * share
    )
    grad_shared_down = jnp.transpose(got_shared[:, :, 2], (0, 2, 1)).reshape(
        groups * share, features // groups
    )

    grad_mixed = (
        contract(grad_attn, w_out, 1, 1)
        .astype(jnp.bfloat16)
        .reshape(seq_rows, heads_here, head_dim)
    )
    again_probs = jnp.exp(attn_scores() - log_total)
    grad_values = jnp.einsum(
        "hqk,qhd->khd",
        again_probs.astype(jnp.bfloat16),
        grad_mixed,
        preferred_element_type=jnp.float32,
    )
    grad_probs_attn = jnp.einsum(
        "qhd,khd->hqk", grad_mixed, value_rows, preferred_element_type=jnp.float32
    )
    grad_scores = again_probs * (
        grad_probs_attn - jnp.sum(again_probs * grad_probs_attn, axis=-1, keepdims=True)
    )
    grad_scores = grad_scores.astype(jnp.bfloat16)
    grad_queries = (
        jnp.einsum("hqk,khd->qhd", grad_scores, key_rows, preferred_element_type=jnp.float32)
        * score_scale
    )
    grad_keys = (
        jnp.einsum("hqk,qhd->khd", grad_scores, queries, preferred_element_type=jnp.float32)
        * score_scale
    )
    grad_pre = jnp.stack(
        [
            rotate_backward(grad_queries, cosine_table, sine_table),
            rotate_backward(grad_keys, cosine_table, sine_table),
            grad_values,
        ]
    )
    grad_pre = grad_pre.reshape(3, seq_rows, -1).astype(jnp.bfloat16)
    low_one_part = jnp.einsum("cle,cde->ld", grad_pre, w_qkv, preferred_element_type=jnp.float32)
    grad_norm_one = jnp.sum(low_one_part * unit_one, axis=0)
    grad_low_one = lane_scatter_sum(low_one_part.astype(jnp.bfloat16), lanes)
    grad_bias = jnp.sum(grad_pre.astype(jnp.float32), axis=1)
    heads_width = grad_bias.shape[1]
    group_rows = features // groups
    bias_column = jnp.transpose(
        grad_bias.reshape(3 * heads_here, groups, head_dim // groups), (1, 0, 2)
    ).reshape(groups, -1)
    bias_count = bias_column.shape[1]
    bias_column = jnp.pad(bias_column, ((0, 0), (0, group_rows - bias_count))).reshape(-1)
    small = jnp.concatenate(
        [grad_norm_one[None], functools.reduce(jnp.add, small_sums), bias_column[None]], axis=0
    )
    small_count = small.shape[0]
    small = jnp.pad(small, ((0, 128 - small_count), (0, 0))).T
    grad_qkv = [contract(low_one, grad_pre[part], 0, 0) for part in range(3)]
    grad_out_weight = contract(grad_attn, attn_mixed, 0, 0)
    sent_weights = [piece.astype(jnp.bfloat16) for piece in (*grad_qkv, grad_out_weight, small)]
    weights = lax.psum_scatter(
        jnp.concatenate(sent_weights, axis=1), "ep", scatter_dimension=0, tiled=True
    )
    attn_weights = [
        weights[:, part * heads_width : (part + 1) * heads_width].astype(jnp.float32)
        for part in range(4)
    ]
    small_parts = lane_gather(weights[:, 4 * heads_width :].astype(jnp.float32), lanes)
    bias_sum = weights[:bias_count, 4 * heads_width + small_count - 1].astype(jnp.float32)
    bias_sum = bias_sum.reshape(3, heads_here, head_dim // groups)
    small_parts = small_parts.reshape(lanes, group_rows, 128)
    small = functools.reduce(jnp.add, [small_parts[lane] for lane in range(lanes)]).T
    grad_input_norm, _ = rms_backward(grad_low_one, norm1_gain, mine(unit_one), mine(scale_one))
    grad_tokens = grad_hidden + grad_input_norm

    return (
        output_rows,
        grad_tokens,
        small[0],
        jnp.stack(attn_weights[:3]),
        bias_sum,
        attn_weights[3].T,
        small[1],
        small[3 : 3 + experts].T,
        small[2],
        grad_shared_gu,
        grad_shared_down,
        grad_expert_gu[None],
        grad_expert_down[None],
    )


def per_device(*arrays):
    experts, chosen = arrays[6].shape[1], arrays[12].shape[1]
    if experts <= 2 * chosen:
        return dense_device(*arrays)
    return routed_device(*arrays)


def solution(mesh):
    return jax.shard_map(
        per_device,
        mesh=mesh,
        in_specs=(
            P("ep", None),
            P(),
            P(None, None, "tp"),
            P(None, "tp", None),
            P("tp", None),
            P(),
            P(),
            P(),
            P(None, None, "tp"),
            P("tp", None),
            P("ep", None, None, "tp"),
            P("ep", "tp", None),
            P("ep", None),
            P("ep", None),
        ),
        out_specs=(
            P(("ep", "tp"), None),
            P(("ep", "tp"), None),
            P("ep"),
            P(None, "ep", "tp"),
            P(None, "tp", "ep"),
            P("tp", "ep"),
            P("ep"),
            P("ep", None),
            P("ep"),
            P(None, "ep", "tp"),
            P("tp", "ep"),
            P("ep", None, None, "tp"),
            P("ep", "tp", None),
        ),
        check_vma=False,
    )
```
